32 devices in a mesh: mp: 8 (over z, y), rows: 4 (over x, core).
Axes of the slice: x: 2, y: 2, z: 4, core: 2. Of those that a mesh axis runs over, the one named last changes fastest.
Arguments:
- inputs: float32 [1024, 16384], P('rows', 'mp'), may hold values from -6 to 6
- weight: float32 [512, 16384], P('mp'), may hold values from -1.5 to 1.5, as said below
Outputs:
- row_scale: float32 [1024], P('rows')
- product: float32 [512, 1024], P('mp', 'rows')
- normalized: float32 [512, 1024], P('mp')
The draws below stay inside these ranges and needn't reach their ends.
Inputs may be any that keep to these rules, and one draw needn't show every extreme that they name: A weight matrix whose rows carry different scales.
All inputs are finite; a program needn't handle non-finite values. Where the reference program divides by a largest or mean magnitude, that divisor is 1e-20 or more.
Results may differ from the reference program's by a relative error of at most 0.0003.
Values may be sent and summed in bfloat16 or wider, within the bound.
No kernel may reach another device: no remote copies, remote signals or barrier semaphores. Data moves between devices by JAX's collectives and lax.ppermute only.
A program may use at most 64 MiB of HBM per device.

```python
import math
import jax
import jax.numpy as jnp
from jax import lax

INNER = 16384
COLS_DEV = 64
COLS = 512
ROWS = 1024
N_MP = 8


def draw_weight(key, part):
    base_key, spread_key = jax.random.split(jax.random.fold_in(key, 11))
    columns = jnp.arange(COLS).astype(jnp.float32)
    rising = jnp.sqrt(1.0 + 2.0 * columns / COLS)
    base = jnp.clip(jax.random.normal(base_key, (COLS, INNER), jnp.float32), -6.0, 6.0)
    spread = jnp.exp(jax.random.uniform(spread_key, (COLS,), jnp.float32, 0.0, math.log(10.0)))
    return (base * (spread * rising)[:, None] / 72.0).astype(jnp.float32)


def levels(stream_key, extent, shards, low, top_value):
    level, own = 1.0, jax.random.fold_in(stream_key, 6)
    for axis_at, blocks in shards:
        draws = jnp.exp(jax.random.uniform(jax.random.fold_in(own, axis_at), (blocks,), jnp.float32, low / len(shards), top_value / len(shards)))
        level = level * jnp.repeat(draws, extent[axis_at] // blocks).reshape([-1 if axis == axis_at else 1 for axis in range(len(extent))])
    return level


def scatter_about(rng, shape, width, reach, pieces=(), held_as=jnp.bfloat16):
    level = levels(rng, shape, pieces, -0.22, 0.18) if pieces else 1.0
    entries = jax.random.normal(rng, shape, jnp.float32) * width * level
    return jnp.minimum(jnp.maximum(entries, -reach), reach).astype(held_as)


def setup_inputs(seed: int = 0) -> dict:
    arg_keys = jax.random.split(jax.random.key(seed), 3)
    inputs = scatter_about(arg_keys[0], (ROWS, INNER), 1.0, 6.0, ((0, 4), (1, 8)), jnp.float32)
    weight = draw_weight(jax.random.fold_in(arg_keys[2], 71), 0)
    return dict(inputs=inputs, weight=weight)


epsilon = 1e-06

def split_two(values):
    scaled = values * 128.0
    first = jnp.floor(scaled)
    second = jnp.floor((scaled - first) * 256.0)
    return (first, second)

def reference(inputs, weight):
    row_scale = lax.optimization_barrier(jnp.max(jnp.abs(inputs), axis=1)) + epsilon
    x_parts = split_two(inputs / row_scale[:, None])
    blocks = weight.reshape(N_MP, COLS_DEV, INNER)
    highest = lax.Precision.HIGHEST

    def column_block(w_block):
        col_scale = lax.optimization_barrier(jnp.max(jnp.abs(w_block), axis=1)) + epsilon
        w_parts = split_two(w_block / col_scale[:, None])
        combined = jnp.dot(w_parts[0] + w_parts[1] / 256.0, x_parts[0].T, precision=highest)
        combined = combined + jnp.dot(w_parts[0], x_parts[1].T, precision=highest) / 256.0
        return combined * col_scale[:, None]
    combined = lax.map(column_block, blocks)
    product = combined.reshape(COLS, ROWS) * row_scale[None, :] / 16384.0
    mean_square = lax.optimization_barrier(jnp.mean(product * product, axis=0))
    normalized = product * lax.rsqrt(mean_square + epsilon)[None, :]
    return (row_scale, product, normalized)
```

```python
import jax
import jax.numpy as jnp
from jax import lax
from jax.sharding import PartitionSpec as P

epsilon = 1e-06


def split_two(values):
    scaled = values * 128.0
    first = jnp.floor(scaled)
    second = jnp.floor((scaled - first) * 256.0)
    return first, second


def matmul(w_side, x_side):
    return lax.dot_general(
        w_side, x_side, (((1,), (1,)), ((), ())), preferred_element_type=jnp.float32
    )


def unite(first, second):
    return first * 256.0 + second


def part_again(united):
    first = jnp.floor(united * (1.0 / 256.0))
    second = united - first * 256.0
    return first.astype(jnp.bfloat16), second.astype(jnp.bfloat16)


def partial_rows(united, x_parts):
    w_first, w_second = part_again(united)
    level_zero = matmul(w_first, x_parts[0])
    level_one = matmul(w_first, x_parts[1]) + matmul(w_second, x_parts[0])
    return level_zero + level_one / 256.0


def per_device(inputs, weight):
    n_mp = lax.axis_size("mp")
    n_rows = lax.axis_size("rows")
    at = lax.axis_index("rows")
    cols, inner = weight.shape
    rows, block = inputs.shape
    share = cols // n_rows

    mine = lax.dynamic_slice_in_dim(weight, at * share, share, axis=0)
    mine_scale = jnp.max(jnp.abs(mine), axis=1) + epsilon
    united = unite(*split_two(mine / mine_scale[:, None]))
    send = united.reshape(share, n_mp, block).transpose(1, 0, 2)
    moved = lax.all_to_all(send, "mp", split_axis=0, concat_axis=0, tiled=True)
    held = [moved.reshape(n_mp * share, block)]
    step = n_rows // 2
    order = [0]
    while step:
        pairs = [(i, i ^ step) for i in range(n_rows)]
        held = held + [lax.ppermute(part, "rows", pairs) for part in held]
        order = order + [spot ^ step for spot in order]
        step //= 2

    row_max = lax.all_gather(jnp.max(jnp.abs(inputs), axis=1), "mp")
    row_scale = jnp.max(row_max, axis=0) + epsilon
    x_parts = tuple(
        part.astype(jnp.bfloat16) for part in split_two(inputs / row_scale[:, None])
    )
    terms = [partial_rows(part, x_parts).reshape(n_mp, 1, share, rows) for part in held]
    blocks = lax.all_to_all(
        jnp.concatenate(terms, axis=1), "mp", split_axis=0, concat_axis=0, tiled=True
    )
    combined = jnp.sum(blocks, axis=0)
    spots = [order.index(i) for i in range(n_rows)]
    step = 1
    while step < n_rows:
        flipped = jnp.stack([combined[order.index(order[i] ^ step)] for i in range(n_rows)])
        combined = jnp.where((at & step) != 0, flipped, combined)
        step *= 2
    combined = jnp.concatenate([combined[i] for i in spots], axis=0)

    col_scale = jnp.max(jnp.abs(weight), axis=1) + epsilon
    product = combined * col_scale[:, None] * row_scale[None, :] / inner
    squares = lax.all_gather(jnp.sum(product * product, axis=0), ("mp", "rows"))
    squares = jnp.sum(squares.reshape(n_mp, n_rows, rows), axis=0)
    mean_square = squares / (cols * n_mp)
    inverse = lax.rsqrt(mean_square + epsilon)
    gathered = lax.all_gather(product, "rows")
    normalized = (gathered * inverse[:, None, :]).transpose(1, 0, 2)
    return row_scale, product, normalized.reshape(cols, n_rows * rows)


def solution(mesh):
    return jax.shard_map(
        per_device,
        mesh=mesh,
        in_specs=(P("rows", "mp"), P("mp", None)),
        out_specs=(P("rows"), P("mp", "rows"), P("mp", None)),
        check_vma=False,
    )
```

```python
import jax
import jax.numpy as jnp
from jax import lax
from jax.sharding import PartitionSpec as P

epsilon = 1e-06


def split_two(values):
    scaled = values * 128.0
    first = jnp.floor(scaled)
    second = jnp.floor((scaled - first) * 256.0)
    return first, second


def matmul(w_side, x_side):
    return lax.dot_general(
        w_side, x_side, (((1,), (1,)), ((), ())), preferred_element_type=jnp.float32
    )


def encode(united):
    power = (jnp.abs(united) + 512.0) * (1.0 / 4096.0)
    for _ in range(5):
        power = power * power
    return jnp.where(united < 0, -power, power).astype(jnp.bfloat16)


def decode(code):
    code = code.astype(jnp.float32)
    root = jnp.exp2(jnp.log2(jnp.abs(code)) * (1.0 / 32.0))
    size = jnp.round(root * 4096.0 - 512.0)
    united = jnp.where(code < 0, -size, size)
    first = jnp.floor(united * (1.0 / 256.0))
    second = united - first * 256.0
    return first.astype(jnp.bfloat16), second.astype(jnp.bfloat16)


def partial_rows(code, x_parts):
    w_first, w_second = decode(code)
    level_zero = matmul(w_first, x_parts[0])
    level_one = matmul(w_first, x_parts[1]) + matmul(w_second, x_parts[0])
    return level_zero + level_one / 256.0


def swap(value, axis, step):
    size = lax.axis_size(axis)
    return lax.ppermute(value, axis, [(i, i ^ step) for i in range(size)])


def powers(size):
    steps, step = [], 1
    while step < size:
        steps.append(step)
        step *= 2
    return steps


def all_over(value, axis, combine):
    for step in powers(lax.axis_size(axis)):
        value = combine(value, swap(value, axis, step))
    return value


def scatter_sum(value, axis, steps):
    at = lax.axis_index(axis)
    bits = powers(lax.axis_size(axis))[::-1]
    value = value.reshape((2,) * len(bits) + value.shape[1:])
    for step in steps:
        dim = bits.index(step)
        low, high = jnp.split(value, 2, axis=dim)
        upper = (at & step) != 0
        away = jnp.where(upper, low, high)
        kept = jnp.where(upper, high, low)
        value = kept + swap(away, axis, step)
    return value.reshape(value.shape[len(bits):])


def per_device(inputs, weight):
    n_mp = lax.axis_size("mp")
    n_rows = lax.axis_size("rows")
    at = lax.axis_index("rows")
    cols, inner = weight.shape
    rows, block = inputs.shape
    share = cols // n_rows

    row_scale = all_over(jnp.max(jnp.abs(inputs), axis=1), "mp", jnp.maximum) + epsilon

    mine = lax.dynamic_slice_in_dim(weight, at * share, share, axis=0)
    mine_scale = jnp.max(jnp.abs(mine), axis=1) + epsilon
    first, second = split_two(mine / mine_scale[:, None])
    send = encode(first * 256.0 + second).reshape(share, n_mp, block).transpose(1, 0, 2)
    moved = lax.all_to_all(send, "mp", split_axis=0, concat_axis=0, tiled=True)
    held = [moved.reshape(n_mp * share, block)]
    order = [0]
    for step in powers(n_rows)[::-1]:
        held = held + [swap(part, "rows", step) for part in held]
        order = order + [spot ^ step for spot in order]

    x_parts = tuple(
        part.astype(jnp.bfloat16) for part in split_two(inputs / row_scale[:, None])
    )
    terms = jnp.concatenate(
        [partial_rows(part, x_parts).reshape(n_mp, 1, share, rows) for part in held], axis=1
    )
    steps = powers(n_mp)
    turned = steps[1:2] + steps[:1] + steps[2:]
    half = rows // 2
    combined = jnp.concatenate(
        [
            scatter_sum(terms[..., :half], "mp", steps),
            scatter_sum(terms[..., half:], "mp", turned),
        ],
        axis=-1,
    )
    for step in powers(n_rows):
        flipped = jnp.stack([combined[order.index(spot ^ step)] for spot in order])
        combined = jnp.where((at & step) != 0, flipped, combined)
    combined = jnp.concatenate([combined[order.index(i)] for i in range(n_rows)], axis=0)

    col_scale = jnp.max(jnp.abs(weight), axis=1) + epsilon
    product = combined * col_scale[:, None] * row_scale[None, :] / inner
    squares = all_over(jnp.sum(product * product, axis=0), "mp", jnp.add)
    inverse = lax.rsqrt(squares / (cols * n_mp) + epsilon)

    def everyone(value):
        return [value] + [swap(value, "rows", away) for away in range(1, n_rows)]

    scaled = [a * b[None, :] for a, b in zip(everyone(product), everyone(inverse))]
    for step in powers(n_rows):
        upper = (at & step) != 0
        scaled = [jnp.where(upper, scaled[i ^ step], scaled[i]) for i in range(n_rows)]
    return row_scale, product, jnp.concatenate(scaled, axis=1)


def solution(mesh):
    return jax.shard_map(
        per_device,
        mesh=mesh,
        in_specs=(P("rows", "mp"), P("mp", None)),
        out_specs=(P("rows"), P("mp", "rows"), P("mp", None)),
        check_vma=False,
    )
```
